32 devices in a mesh: rep: 1, dp: 32 (over x, y, z, core).
Axes of the slice: x: 2, y: 2, z: 4, core: 2. Of those that a mesh axis runs over, the one named last changes fastest.
Arguments:
- x: bfloat16 [32, 2048, 896], P(('rep', 'dp'))
- dy: bfloat16 [32, 2048, 896], P(('rep', 'dp'))
- wq: bfloat16 [2, 896, 896], P(None, 'dp')
- wk: bfloat16 [2, 896, 128], P(None, 'dp')
- wv: bfloat16 [2, 896, 128], P(None, 'dp')
- wo: bfloat16 [2, 896, 896], P(None, 'dp')
- w_gate: bfloat16 [2, 896, 2560], P(None, 'dp')
- w_up: bfloat16 [2, 896, 2560], P(None, 'dp')
- w_down: bfloat16 [2, 2560, 896], P(None, 'dp')
Outputs:
- output 1: bfloat16 [32, 2048, 896], P(('rep', 'dp'))
- output 2: bfloat16 [2, 896, 896], P('rep', 'dp')
- output 3: bfloat16 [2, 896, 128], P('rep', 'dp')
- output 4: bfloat16 [2, 896, 128], P('rep', 'dp')
- output 5: bfloat16 [2, 896, 896], P('rep', 'dp')
- output 6: bfloat16 [2, 896, 2560], P('rep', 'dp')
- output 7: bfloat16 [2, 896, 2560], P('rep', 'dp')
- output 8: bfloat16 [2, 2560, 896], P('rep', 'dp')
All inputs are finite; a program needn't handle non-finite values.
Results may differ from the reference program's by a relative error of at most 0.0287.
Values are sent between devices in bfloat16 or wider.
A program may use at most 2 GiB of HBM per device.

```python
import jax
import jax.numpy as jnp
from jax import lax

SEQUENCES = 32
TOKENS = 2048
D = 896
HEADS = 7
KV_HEADS = 1
HEAD = 128
FF = 2560
LAYERS = 2
THETA = 10000
NAMES = ("wq", "wk", "wv", "wo", "w_gate", "w_up", "w_down")
SHAPES = {
    "wq": (LAYERS, D, HEADS * HEAD),
    "wk": (LAYERS, D, KV_HEADS * HEAD),
    "wv": (LAYERS, D, KV_HEADS * HEAD),
    "wo": (LAYERS, HEADS * HEAD, D),
    "w_gate": (LAYERS, D, FF),
    "w_up": (LAYERS, D, FF),
    "w_down": (LAYERS, FF, D),
}


def bump(key, n, height):
    away = (jnp.arange(n, dtype=jnp.int32) - jax.random.randint(key, (), 0, n, jnp.int32)) % n
    return jnp.where(away < n // 8, height, 1.0)


def together(key, own, strength):
    shared = jax.random.normal(key, own.shape[1:], jnp.float32)
    return (own + strength * shared) * lax.rsqrt(1 + strength * strength)


def setup_inputs(seed: int = 0, part: int = 0) -> dict:
    kx, kdy, ka, kb, kz, kf, kh, kl, *keys = jax.random.split(jax.random.key(seed), 8 + 3 * len(NAMES))
    kx, kdy, ka, kb = (jax.random.fold_in(k, part) for k in (kx, kdy, ka, kb))
    kw, km, kv = (keys[i::3] for i in range(3))
    shape = (SEQUENCES, TOKENS, D)
    much_x, much_dy = jax.random.uniform(kz, (2,), jnp.float32, 0.0, 1.0)
    loud = 2.0 ** jax.random.uniform(jax.random.fold_in(kz, 1), (), jnp.float32, -1.0, 2.0)
    layers = 2.0 ** jax.random.uniform(kl, (LAYERS, 1, 1), jnp.float32, -1.0, 1.0)
    times = {"wq": 1.0, "wk": 1.0, "wv": 2.0, "wo": layers, "w_gate": 1.0, "w_up": bump(kh, FF, 4.0), "w_down": layers}
    x = together(ka, jax.random.normal(kx, shape, jnp.float32), much_x) * bump(kf, D, 4.0)
    dy = together(kb, jax.random.normal(kdy, shape, jnp.float32), much_dy)
    drawn = {"x": x.astype(jnp.bfloat16), "dy": (loud * dy * (SEQUENCES * TOKENS) ** -0.5).astype(jnp.bfloat16)}
    for key, name in zip(kw, NAMES, strict=True):
        drawn[name] = (jax.random.normal(key, SHAPES[name], jnp.float32) * SHAPES[name][1] ** -0.5 * times[name]).astype(jnp.bfloat16)
    return drawn


def matmul(a, w):
    return jnp.dot(a, w, preferred_element_type=jnp.float32).astype(jnp.bfloat16)


def normed(h):
    wide = h.astype(jnp.float32)
    scale = lax.rsqrt(jnp.mean(wide**2, -1, keepdims=True) + 1e-6)
    return (wide * scale).astype(jnp.bfloat16)


def turned(t, theta):
    half = t.shape[-1] // 2
    angle = jnp.arange(t.shape[0], dtype=jnp.float32)[:, None] * theta ** (-jnp.arange(half, dtype=jnp.float32) / half)
    cos, sin = jnp.cos(angle)[:, None], jnp.sin(angle)[:, None]
    a, b = t[..., :half].astype(jnp.float32), t[..., half:].astype(jnp.float32)
    return jnp.concatenate([a * cos - b * sin, b * cos + a * sin], -1).astype(jnp.bfloat16)


def seen_by(q, k, v):
    tokens, kv = q.shape[0], k.shape[1]
    q = q.reshape(tokens, kv, -1, q.shape[-1])
    scores = jnp.einsum("tgsd,ugd->gstu", q.astype(jnp.float32), k.astype(jnp.float32)) * q.shape[-1] ** -0.5
    place = jnp.arange(tokens)
    weights = jax.nn.softmax(jnp.where(place[:, None] >= place, scores, -jnp.inf), -1).astype(jnp.bfloat16)
    return jnp.einsum("gstu,ugd->tgsd", weights.astype(jnp.float32), v.astype(jnp.float32)).astype(jnp.bfloat16).reshape(tokens, -1)


def layer(h, w):
    a = normed(h)
    q, k = (turned(matmul(a, w[name]).reshape(h.shape[0], -1, HEAD), THETA) for name in ("wq", "wk"))
    h = h + matmul(seen_by(q, k, matmul(a, w["wv"]).reshape(h.shape[0], -1, HEAD)), w["wo"])
    b = normed(h)
    gate = jnp.dot(b, w["w_gate"], preferred_element_type=jnp.float32)
    up = jnp.dot(b, w["w_up"], preferred_element_type=jnp.float32)
    return h + matmul((jax.nn.silu(gate) * up).astype(jnp.bfloat16), w["w_down"])


def stack(weights, h):
    return lax.scan(lambda h, w: (layer(h, w), None), h, weights)[0]


def reference(x, dy, wq, wk, wv, wo, w_gate, w_up, w_down):
    weights = dict(zip(NAMES, (wq, wk, wv, wo, w_gate, w_up, w_down), strict=True))

    def take(so_far, sequence):
        h, by_y = sequence
        _, back = jax.vjp(stack, weights, h)
        by_weights, by_h = back(by_y)
        return jax.tree.map(lambda total, term: total + term.astype(jnp.float32), so_far, by_weights), by_h

    none_yet = {name: jnp.zeros(w.shape, jnp.float32) for name, w in weights.items()}
    by_weights, by_x = lax.scan(take, none_yet, (x, dy))
    return (by_x, *(by_weights[name].astype(jnp.bfloat16) for name in NAMES))
```

```python
import functools

import jax
import jax.numpy as jnp
from jax import lax
from jax.experimental import pallas as pl
from jax.experimental.pallas import tpu as pltpu
from jax.sharding import PartitionSpec as P

HEAD = 128
THETA = 10000
EPS = 1e-6
NEG = -1e30
HIDDEN = 2 * NEG
LOG2E = 1.4426950408889634
VMEM = 60 * 2**20
ROOM = 32
BF16, F32 = jnp.bfloat16, jnp.float32


def _dot(a, b, ca=1, cb=0):
    return lax.dot_general(a, b, (((ca,), (cb,)), ((), ())), preferred_element_type=F32)


def _params(grid, **more):
    return pltpu.CompilerParams(dimension_semantics=("arbitrary",) * grid, vmem_limit_bytes=VMEM, **more)


def _cost(flops, moved, exps=0):
    return pl.CostEstimate(flops=int(flops), bytes_accessed=int(moved), transcendentals=int(exps))


def _once(shape, index):
    return pl.BlockSpec(shape, lambda *_: index, pipeline_mode=pl.Buffered(1))


def _scale(wide):
    return lax.rsqrt(jnp.mean(wide * wide, -1, keepdims=True) + EPS)


def _norm_back(by_out, wide):
    scale = _scale(wide)
    dot = jnp.sum(by_out * wide, -1, keepdims=True)
    return (by_out * scale - wide * (scale * scale * scale * dot * (1 / wide.shape[-1]))).astype(BF16)


def _add(a, b):
    return (a.astype(F32) + b.astype(F32)).astype(BF16)


def _compact_body(got_ref, out_ref, *, count, rows):
    for i in range(count):
        out_ref[i * rows : (i + 1) * rows, :] = got_ref[i, :rows, :]


def compact(got, pieces, rows):
    count, _, width = got.shape
    return pl.pallas_call(
        functools.partial(_compact_body, count=count, rows=rows),
        grid=(pieces,),
        in_specs=[pl.BlockSpec((count, ROOM, width), lambda j: (0, j, 0))],
        out_specs=pl.BlockSpec((count * rows, width), lambda j: (0, j)),
        out_shape=jax.ShapeDtypeStruct((count * rows, pieces * width), BF16),
        compiler_params=_params(1),
        cost_estimate=_cost(2e9, 2 * got.size * 2),
        name="compact",
    )(got)


def _qkv_body(h_ref, w_ref, cos_ref, sin_ref, q_ref, k_ref, v_ref, a_ref, *, heads):
    wide = h_ref[...].astype(F32)
    a = (wide * _scale(wide)).astype(BF16)
    a_ref[...] = a
    cos, sin = cos_ref[...], sin_ref[...]
    out = _dot(a, w_ref[:, : (heads + 2) * HEAD]).astype(BF16)
    for n in range(heads + 1):
        t = out[:, n * HEAD : (n + 1) * HEAD].astype(F32)
        t = (t * cos + pltpu.roll(t, HEAD // 2, 1) * sin).astype(BF16)
        if n < heads:
            q_ref[n] = t
        else:
            k_ref[...] = t
    v_ref[...] = out[:, (heads + 1) * HEAD :]


def qkv_forward(h, w, at, heads, cos, sin, bm=512):
    s, d = h.shape
    rows = pl.BlockSpec((bm, d), lambda i: (i, 0))
    head = pl.BlockSpec((bm, HEAD), lambda i: (i, 0))
    wide = 1280
    return pl.pallas_call(
        functools.partial(_qkv_body, heads=heads),
        grid=(s // bm,),
        in_specs=[rows, _once((d, wide), (0, at // wide)), head, head],
        out_specs=[pl.BlockSpec((heads, bm, HEAD), lambda i: (0, i, 0)), head, head, rows],
        out_shape=[jax.ShapeDtypeStruct((heads, s, HEAD), BF16), jax.ShapeDtypeStruct((s, HEAD), BF16),
                   jax.ShapeDtypeStruct((s, HEAD), BF16), jax.ShapeDtypeStruct((s, d), BF16)],
        compiler_params=_params(1),
        cost_estimate=_cost(2 * s * d * (heads + 2) * HEAD, 16e6),
        name="qkv_forward",
    )(h, w, cos, sin)


def _qkv_back_body(dq_ref, dk_ref, dv_ref, h_ref, dh_ref, w_ref, cos_ref, sin_ref, all_ref, out_ref, *, heads):
    cos, sin = cos_ref[...], sin_ref[...]
    for n in range(heads + 1):
        t = (dq_ref[:, n * HEAD : (n + 1) * HEAD] if n < heads else dk_ref[...]).astype(F32)
        all_ref[:, n * HEAD : (n + 1) * HEAD] = (t * cos - pltpu.roll(t, HEAD // 2, 1) * sin).astype(BF16)
    all_ref[:, (heads + 1) * HEAD :] = dv_ref[...]
    da = _dot(all_ref[...], w_ref[:, : (heads + 2) * HEAD], 1, 1).astype(BF16).astype(F32)
    out_ref[...] = _add(dh_ref[...], _norm_back(da, h_ref[...].astype(F32)))


def qkv_backward(dq, dk, dv, h, dh, w, at, heads, cos, sin, bm=512):
    s, d = h.shape
    rows = pl.BlockSpec((bm, d), lambda i: (i, 0))
    head = pl.BlockSpec((bm, HEAD), lambda i: (i, 0))
    wide = 1280
    all_wide = (heads + 2) * HEAD
    return pl.pallas_call(
        functools.partial(_qkv_back_body, heads=heads),
        grid=(s // bm,),
        in_specs=[rows, head, head, rows, rows, _once((d, wide), (0, at // wide)), head, head],
        out_specs=[pl.BlockSpec((bm, all_wide), lambda i: (i, 0)), rows],
        out_shape=[jax.ShapeDtypeStruct((s, all_wide), BF16), jax.ShapeDtypeStruct((s, d), BF16)],
        compiler_params=_params(1),
        cost_estimate=_cost(2 * s * d * all_wide, 25e6),
        name="qkv_backward",
    )(dq, dk, dv, h, dh, w, cos, sin)


def _gap(bk, cols, bq):
    return lax.rem(lax.broadcasted_iota(jnp.int32, (bk, cols), 1), bq) - lax.broadcasted_iota(jnp.int32, (bk, cols), 0)


def _attend_body(q_ref, k_ref, v_ref, o_ref, lse_ref, top_s, mix_s, gap_s, *, scale, bq, bk):
    g = q_ref.shape[0]
    cols = g * bq
    iq = pl.program_id(0)
    e = scale * LOG2E

    @pl.when(iq == 0)
    def _():
        gap_s[...] = _gap(bk, bq, bq)

    top_s[...] = jnp.full((1, cols), NEG, F32)
    mix_s[...] = jnp.zeros((HEAD + 8, cols), F32)
    ones = jnp.ones((8, bk), BF16)

    def block(j, masked):
        here = pl.ds(pl.multiple_of(j * bk, bk), bk)
        keys = k_ref[here, :]
        scores = [_dot(keys, q_ref[n], 1, 1) for n in range(g)]
        ok = gap_s[...] >= j * bk - iq * bq if masked else None
        weights, keeps = [], []
        for n, s in enumerate(scores):
            at = slice(n * bq, (n + 1) * bq)
            if masked:
                s = jnp.where(ok, s, HIDDEN)
            old = top_s[:, at]
            top = jnp.maximum(old, s.max(axis=0, keepdims=True))
            top_s[:, at] = top
            weights.append(jnp.exp2((s - top) * e).astype(BF16))
            keeps.append(jnp.exp2((old - top) * e))
        values = jnp.concatenate([v_ref[here, :].T, ones], axis=0)
        for n, (p, keep) in enumerate(zip(weights, keeps)):
            at = slice(n * bq, (n + 1) * bq)
            mix_s[:, at] = mix_s[:, at] * keep + _dot(values, p)

    whole, last = lax.div(iq * bq + 1, bk), lax.div(iq * bq + bq - 1 + bk, bk)
    lax.fori_loop(0, whole, lambda j, _: block(j, False), None)
    lax.fori_loop(whole, last, lambda j, _: block(j, True), None)
    for n in range(g):
        at = slice(n * bq, (n + 1) * bq)
        total = mix_s[HEAD : HEAD + 1, at]
        o_ref[:, n * HEAD : (n + 1) * HEAD] = (mix_s[:HEAD, at] * (1 / total)).T.astype(BF16)
        lse_ref[n : n + 1, :] = top_s[:, at] * scale + jnp.log(total)


def attend(q, k, v, bq=512, bk=512):
    g, s, d = q.shape
    whole = _once((s, d), (0, 0))
    return pl.pallas_call(
        functools.partial(_attend_body, scale=d**-0.5, bq=bq, bk=bk),
        grid=(s // bq,),
        in_specs=[pl.BlockSpec((g, bq, d), lambda i: (0, i, 0)), whole, whole],
        out_specs=[pl.BlockSpec((bq, g * d), lambda i: (i, 0)), pl.BlockSpec((g, bq), lambda i: (0, i))],
        out_shape=[jax.ShapeDtypeStruct((s, g * d), BF16), jax.ShapeDtypeStruct((g, s), F32)],
        scratch_shapes=[pltpu.VMEM((1, g * bq), F32), pltpu.VMEM((d + 8, g * bq), F32), pltpu.VMEM((bk, bq), jnp.int32)],
        compiler_params=_params(1),
        cost_estimate=_cost(8 * g * s * s * d, 8e6, g * s * s),
        name="attend",
    )(q, k, v)


def _attend_back_body(q_ref, k_ref, v_ref, do_ref, o_ref, lse_ref, dq_ref, dk_ref, dv_ref, dq_s, dk_s, dv_s, gap_s, *, scale, bq, bk):
    g = q_ref.shape[0]
    iq = pl.program_id(0)
    e = scale * LOG2E

    @pl.when(iq == 0)
    def _():
        gap_s[...] = _gap(bk, bq, bq)
        dk_s[...] = jnp.zeros_like(dk_s)
        dv_s[...] = jnp.zeros_like(dv_s)

    dq_s[...] = jnp.zeros_like(dq_s)
    ones = jnp.ones((8, HEAD), BF16)
    lses, deltas = [], []
    for n in range(g):
        lses.append(lse_ref[n : n + 1, :] * LOG2E)
        both = do_ref[:, n * HEAD : (n + 1) * HEAD].astype(F32) * o_ref[:, n * HEAD : (n + 1) * HEAD].astype(F32)
        high = both.astype(BF16)
        rest = both - high.astype(F32)
        low = rest.astype(BF16)
        last = (rest - low.astype(F32)).astype(BF16)
        deltas.append((_dot(ones, high, 1, 1) + _dot(ones, low, 1, 1) + _dot(ones, last, 1, 1))[:1, :])

    def block(j, masked):
        here = pl.ds(pl.multiple_of(j * bk, bk), bk)
        keys, values = k_ref[here, :], v_ref[here, :]
        dos = [do_ref[:, n * HEAD : (n + 1) * HEAD] for n in range(g)]
        scores = [_dot(keys, q_ref[n], 1, 1) for n in range(g)]
        dps = [_dot(values, x, 1, 1) for x in dos]
        ok = gap_s[...] >= j * bk - iq * bq if masked else None
        turned = keys.T
        for n in range(g):
            p = jnp.exp2(scores[n] * e - lses[n])
            if masked:
                p = jnp.where(ok, p, 0.0)
            ds = (p * (dps[n] - deltas[n])).astype(BF16)
            dv_s[here, :] += _dot(p.astype(BF16), dos[n])
            dk_s[here, :] += _dot(ds, q_ref[n])
            dq_s[:, n * bq : (n + 1) * bq] += _dot(turned, ds)

    whole, last = lax.div(iq * bq + 1, bk), lax.div(iq * bq + bq - 1 + bk, bk)
    lax.fori_loop(0, whole, lambda j, _: block(j, False), None)
    lax.fori_loop(whole, last, lambda j, _: block(j, True), None)
    for n in range(g):
        dq_ref[:, n * HEAD : (n + 1) * HEAD] = (dq_s[:, n * bq : (n + 1) * bq] * scale).T.astype(BF16)

    @pl.when(iq == pl.num_programs(0) - 1)
    def _():
        dk_ref[...] = (dk_s[...] * scale).astype(BF16)
        dv_ref[...] = dv_s[...].astype(BF16)


def attend_back(q, k, v, do, o, lse, bq=256, bk=512):
    g, s, d = q.shape
    whole = _once((s, d), (0, 0))
    rows = pl.BlockSpec((bq, g * d), lambda i: (i, 0))
    return pl.pallas_call(
        functools.partial(_attend_back_body, scale=d**-0.5, bq=bq, bk=bk),
        grid=(s // bq,),
        in_specs=[pl.BlockSpec((g, bq, d), lambda i: (0, i, 0)), whole, whole, rows, rows, pl.BlockSpec((g, bq), lambda i: (0, i))],
        out_specs=[rows, pl.BlockSpec((s, d), lambda i: (0, 0)), pl.BlockSpec((s, d), lambda i: (0, 0))],
        out_shape=[jax.ShapeDtypeStruct((s, g * d), BF16), jax.ShapeDtypeStruct((s, d), BF16), jax.ShapeDtypeStruct((s, d), BF16)],
        scratch_shapes=[pltpu.VMEM((d, g * bq), F32), pltpu.VMEM((s, d), F32), pltpu.VMEM((s, d), F32), pltpu.VMEM((bk, bq), jnp.int32)],
        compiler_params=_params(1),
        cost_estimate=_cost(10 * g * s * s * d, 16e6, g * s * s),
        name="attend_back",
    )(q, k, v, do, o, lse)


def _fetch_down(got_ref, down_s, sem, at, rows):
    @pl.when(pl.program_id(0) == 0)
    def _():
        copy = pltpu.make_async_copy(got_ref.at[:, pl.ds(at, rows), :], down_s, sem)
        copy.start()
        copy.wait()


def _mlp_body(o_ref, h_ref, gu_ref, wo_ref, got_ref, h2_ref, b_ref, g_ref, u_ref, act_ref, out_ref, down_s, sem, *, at, rows, part):
    _fetch_down(got_ref, down_s, sem, at, rows)
    ff = g_ref.shape[1]
    h2 = _add(h_ref[...], _dot(o_ref[...], wo_ref[...]).astype(BF16))
    h2_ref[...] = h2
    wide = h2.astype(F32)
    b = (wide * _scale(wide)).astype(BF16)
    b_ref[...] = b
    total = jnp.zeros(out_ref.shape, F32)
    step = part * rows
    for j in range(ff // step):
        here = slice(j * step, (j + 1) * step)
        gate = _dot(b, gu_ref[:, here])
        up = _dot(b, gu_ref[:, ff + j * step : ff + (j + 1) * step])
        g_ref[:, here] = gate
        u_ref[:, here] = up
        act = (gate * lax.logistic(gate) * up).astype(BF16)
        act_ref[:, here] = act
        total += _dot(act, down_s[j * part : (j + 1) * part].reshape(step, -1))
    out_ref[...] = _add(h2, total.astype(BF16))


def mlp_forward(o, h, w, got, at, rows, ff, bm=256, part=8):
    s, d = h.shape
    row = lambda n: pl.BlockSpec((bm, n), lambda i: (i, 0))
    sds = lambda n, t: jax.ShapeDtypeStruct((s, n), t)
    return pl.pallas_call(
        functools.partial(_mlp_body, at=at, rows=rows, part=part),
        grid=(s // bm,),
        in_specs=[row(d), row(d), _once((d, 2 * ff), (0, 0)), _once((d, d), (0, w.shape[1] // d - 1)), pl.BlockSpec(memory_space=pltpu.HBM)],
        out_specs=[row(d), row(d), row(ff), row(ff), row(ff), row(d)],
        out_shape=[sds(d, BF16), sds(d, BF16), sds(ff, F32), sds(ff, F32), sds(ff, BF16), sds(d, BF16)],
        scratch_shapes=[pltpu.VMEM((got.shape[0], rows, d), BF16), pltpu.SemaphoreType.DMA],
        compiler_params=_params(1),
        cost_estimate=_cost(2 * s * d * (3 * ff + d), 85e6, s * ff),
        name="mlp_forward",
    )(o, h, w, w, got)


def _mlp_back_body(dy_ref, g_ref, u_ref, h2_ref, gu_ref, wo_ref, got_ref, dg_ref, du_ref, dh_ref, do_ref, down_s, sem, *, at, rows, part):
    _fetch_down(got_ref, down_s, sem, at, rows)
    ff = g_ref.shape[1]
    dy = dy_ref[...]
    total = jnp.zeros(dh_ref.shape, F32)
    step = part * rows
    for j in range(ff // step):
        here = slice(j * step, (j + 1) * step)
        da = _dot(dy, down_s[j * part : (j + 1) * part].reshape(step, -1), 1, 1).astype(BF16).astype(F32)
        gate, up = g_ref[:, here], u_ref[:, here]
        s = lax.logistic(gate)
        dg = (da * up * (s * (1 + gate * (1 - s)))).astype(BF16)
        du = (da * (gate * s)).astype(BF16)
        dg_ref[:, here] = dg
        du_ref[:, here] = du
        total += _dot(dg, gu_ref[:, here], 1, 1) + _dot(du, gu_ref[:, ff + j * step : ff + (j + 1) * step], 1, 1)
    dh = _add(dy, _norm_back(total.astype(BF16).astype(F32), h2_ref[...].astype(F32)))
    dh_ref[...] = dh
    do_ref[...] = _dot(dh, wo_ref[...], 1, 1).astype(BF16)


def mlp_backward(dy, g, u, h2, w, got, at, rows, bm=256, part=8):
    s, d = dy.shape
    ff = g.shape[1]
    row = lambda n: pl.BlockSpec((bm, n), lambda i: (i, 0))
    sds = lambda n: jax.ShapeDtypeStruct((s, n), BF16)
    return pl.pallas_call(
        functools.partial(_mlp_back_body, at=at, rows=rows, part=part),
        grid=(s // bm,),
        in_specs=[row(d), row(ff), row(ff), row(d), _once((d, 2 * ff), (0, 0)), _once((d, d), (0, w.shape[1] // d - 1)),
                  pl.BlockSpec(memory_space=pltpu.HBM)],
        out_specs=[row(ff), row(ff), row(d), row(d)],
        out_shape=[sds(ff), sds(ff), sds(d), sds(d)],
        scratch_shapes=[pltpu.VMEM((got.shape[0], rows, d), BF16), pltpu.SemaphoreType.DMA],
        compiler_params=_params(1),
        cost_estimate=_cost(2 * s * d * (3 * ff + d), 95e6, s * ff),
        name="mlp_backward",
    )(dy, g, u, h2, w, w, got)


def _place(place_ref, i, value, keep_ref, send_ref, rows):
    at = place_ref[i]
    half = keep_ref.shape[0]

    @pl.when(at < half)
    def _():
        keep_ref[at, :rows, :] = value

    @pl.when(at >= half)
    def _():
        send_ref[at - half, :rows, :] = value


def _grad_wide_body(place_ref, a_ref, *rest, rows, steps):
    *g_refs, keep_ref, send_ref, turned_s, sum_s = rest

    @pl.when(pl.program_id(0) == 0)
    def _():
        turned_s[...] = a_ref[...].T

    for n, g_ref in enumerate(g_refs):

        @pl.when(lax.div(pl.program_id(0), steps) == n)
        def _():
            sum_s[...] = _dot(turned_s[...], g_ref[...])

    room = keep_ref.shape[1]
    if rows < room:
        blank = jnp.zeros((keep_ref.shape[0], room - rows, keep_ref.shape[2]), BF16)
        keep_ref[:, rows:, :] = blank
        send_ref[:, rows:, :] = blank
    for i in range(2 * keep_ref.shape[0]):
        _place(place_ref, i, sum_s[i * rows : (i + 1) * rows, :].astype(BF16), keep_ref, send_ref, rows)


def grad_wide(place, a, *gs, rows, bn):
    s, m = a.shape
    steps = gs[0].shape[1] // bn
    n = sum(g.shape[1] for g in gs)
    half = m // rows // 2
    out = pl.BlockSpec((half, ROOM, bn), lambda j, _: (0, 0, j))
    shape = jax.ShapeDtypeStruct((half, ROOM, n), BF16)
    ins = [pl.BlockSpec((s, bn), lambda j, _, i=i: (0, jnp.clip(j - i * steps, 0, steps - 1))) for i in range(len(gs))]
    return pl.pallas_call(
        functools.partial(_grad_wide_body, rows=rows, steps=steps),
        grid_spec=pltpu.PrefetchScalarGridSpec(
            num_scalar_prefetch=1, grid=(n // bn,),
            in_specs=[_once((s, m), (0, 0)), *ins],
            out_specs=[out, out],
            scratch_shapes=[pltpu.VMEM((m, s), BF16), pltpu.VMEM((m, bn), F32)]),
        out_shape=[shape, shape],
        compiler_params=_params(1),
        cost_estimate=_cost(2 * s * m * n, 2 * (s * m + s * n + m * n)),
        name="grad_wide",
    )(place, a, *gs)


def _grad_tall_body(place_ref, a_ref, g_ref, keep_ref, send_ref, sum_s, *, rows):
    sum_s[...] = _dot(a_ref[...].T, g_ref[...])
    count = sum_s.shape[0] // rows
    for i in range(count):
        _place(place_ref, pl.program_id(0) * count + i, sum_s[i * rows : (i + 1) * rows, :].astype(BF16), keep_ref, send_ref, rows)


def grad_tall(place, a, g, rows, bm):
    s, m = a.shape
    n = g.shape[1]
    half = m // rows // 2
    out = pl.BlockSpec((half, rows, n), lambda j, _: (0, 0, 0))
    shape = jax.ShapeDtypeStruct((half, rows, n), BF16)
    return pl.pallas_call(
        functools.partial(_grad_tall_body, rows=rows),
        grid_spec=pltpu.PrefetchScalarGridSpec(
            num_scalar_prefetch=1, grid=(m // bm,),
            in_specs=[pl.BlockSpec((s, bm), lambda j, _: (0, j)), _once((s, n), (0, 0))],
            out_specs=[out, out],
            scratch_shapes=[pltpu.VMEM((bm, n), F32)]),
        out_shape=[shape, shape],
        compiler_params=_params(1),
        cost_estimate=_cost(2 * s * m * n, 2 * (s * m + s * n + m * n)),
        name="grad_tall",
    )(place, a, g)


def solution(mesh):
    size = mesh.shape["dp"]
    CORE, ZNEAR, ZFAR, Y, X = 1, 2, 4, 8, 16
    ORDERS = {"gate_up": (CORE, X, Y, ZNEAR, ZFAR), "down": (CORE, ZNEAR, ZFAR, Y, X), "o": (CORE, Y, X, ZNEAR, ZFAR),
              "qkv": (CORE, Y, X, ZNEAR, ZFAR)}

    def place(order, me):
        away = jnp.arange(size, dtype=jnp.int32) ^ me
        at = jnp.zeros_like(away)
        for bit in order:
            at = 2 * at + ((away & bit) != 0)
        return at

    class Sums:
        def __init__(self):
            self.under_way, self.done, self.last = {}, {}, []

        def begin(self, name, order, keep, send):
            self.under_way[name] = [order, 0, keep, send, None]

        def advance(self):
            for name, state in list(self.under_way.items()):
                order, number, keep, send, got = state
                if got is None:
                    continue
                half = keep.shape[0] // 2
                if half == 0:
                    self.done[name] = _add(keep[0], got[0])
                    del self.under_way[name]
                else:
                    self.under_way[name] = [order, number + 1, _add(keep[:half], got[:half]), _add(keep[half:], got[half:]), None]

        def fence(self, *values):
            names = [name for name, state in self.under_way.items() if state[4] is None]
            values, halves, _ = lax.optimization_barrier((values, [self.under_way[name][2:4] for name in names], self.last))
            for name, (keep, send) in zip(names, halves):
                order, number = self.under_way[name][:2]
                got = lax.ppermute(send, "dp", [(i, i ^ order[number]) for i in range(size)])
                self.under_way[name] = [order, number, keep, send, got]
            return values

        def run(self, kernel, *values, **more):
            self.advance()
            out = kernel(*self.fence(*values), **more)
            self.last = [out[0]]
            return out

        def finish(self):
            while self.under_way:
                self.advance()
                self.fence()

    def step(x, dy, wq, wk, wv, wo, w_gate, w_up, w_down):
        layers, own, d = wq.shape
        heads, ff, tall = wq.shape[2] // HEAD, w_gate.shape[2], w_down.shape[1]
        at_qkv = 2 * ff
        pieces = (2 * ff + wq.shape[2] + 2 * HEAD + d) // d
        s = x.shape[1]
        half = HEAD // 2
        angle = jnp.arange(s, dtype=F32)[:, None] * THETA ** (-jnp.arange(half, dtype=F32) / half)
        cos, sin = jnp.cos(angle), jnp.sin(angle)
        cos, sin = jnp.concatenate([cos, cos], 1), jnp.concatenate([-sin, sin], 1)

        gots = []
        for n in range(layers):
            rows = jnp.concatenate([w_gate[n], w_up[n], wq[n], wk[n], wv[n], wo[n]], 1).reshape(own, pieces, d)
            rows = jnp.pad(rows.transpose(1, 0, 2), ((0, 0), (0, ROOM - own), (0, 0))).reshape(pieces * ROOM, d)
            gots.append(lax.all_gather(jnp.concatenate([rows, w_down[n]], 0), "dp", axis=0))
        at_down = pieces * ROOM

        h, kept, ws = x[0], [], []
        for n in range(layers):
            w = compact(gots[n], pieces, own)
            q, k, v, a = qkv_forward(h, w, at_qkv, heads, cos, sin)
            o, lse = attend(q, k, v)
            h2, b, g, u, act, out = mlp_forward(o, h, w, gots[n], at_down, tall, ff)
            kept.append((h, q, k, v, a, o, lse, h2, b, g, u, act))
            ws.append(w)
            h = out

        me = lax.axis_index("dp")
        places = {name: place(order, me) for name, order in ORDERS.items()}
        by_h, sums = dy[0], Sums()

        def grad(name, n, kernel, *values, **more):
            sums.begin((name, n), ORDERS[name], *sums.run(functools.partial(kernel, places[name]), *values, **more))

        for n in reversed(range(layers)):
            h, q, k, v, a, o, lse, h2, b, g, u, act = kept[n]
            w, got = ws[n], gots[n]
            grad("down", n, grad_tall, act, by_h, rows=tall, bm=640)
            dg, du, dh, do = sums.run(mlp_backward, by_h, g, u, h2, w=w, got=got, at=at_down, rows=tall)
            grad("gate_up", n, grad_wide, b, dg, du, rows=own, bn=512)
            grad("o", n, grad_wide, o, dh, rows=own, bn=896)
            dq, dk, dv = sums.run(attend_back, q, k, v, do, o, lse)
            dqkv, by_h = sums.run(qkv_backward, dq, dk, dv, h, dh, w=w, at=at_qkv, heads=heads, cos=cos, sin=sin)
            grad("qkv", n, grad_wide, a, dqkv, rows=own, bn=384)
        sums.finish()
        cut = heads * HEAD
        per = []
        for n in range(layers):
            qkv, gu = sums.done["qkv", n][:own], sums.done["gate_up", n][:own]
            per.append((qkv[:, :cut], qkv[:, cut : cut + HEAD], qkv[:, cut + HEAD :], sums.done["o", n][:own], gu[:, :ff], gu[:, ff:],
                        sums.done["down", n]))
        return (by_h[None], *(jnp.stack([p[i] for p in per]) for i in range(7)))

    states, cut = P(("rep", "dp"), None, None), P(None, "dp", None)
    return jax.shard_map(
        step,
        mesh=mesh,
        in_specs=(states, states) + (cut,) * 7,
        out_specs=(states,) + (P("rep", "dp", None),) * 7,
        check_vma=False,
    )
```

```python
import functools

import jax
import jax.numpy as jnp
from jax import lax
from jax.experimental import pallas as pl
from jax.experimental.pallas import tpu as pltpu
from jax.sharding import PartitionSpec as P

HEAD = 128
THETA = 10000
EPS = 1e-6
NEG = -1e30
HIDDEN = 2 * NEG
LOG2E = 1.4426950408889634
VMEM = 60 * 2**20
ROOM = 32
BF16, F32 = jnp.bfloat16, jnp.float32


def _dot(a, b, ca=1, cb=0):
    return lax.dot_general(a, b, (((ca,), (cb,)), ((), ())), preferred_element_type=F32)


def _params(grid, **more):
    return pltpu.CompilerParams(dimension_semantics=("arbitrary",) * grid, vmem_limit_bytes=VMEM, **more)


def _cost(flops, moved, exps=0):
    return pl.CostEstimate(flops=int(flops) // 8, bytes_accessed=int(moved), transcendentals=int(exps))


def _once(shape, index):
    return pl.BlockSpec(shape, lambda *_: index, pipeline_mode=pl.Buffered(1))


def _scale(wide):
    return lax.rsqrt(jnp.mean(wide * wide, -1, keepdims=True) + EPS)


def _norm_back(by_out, wide):
    scale = _scale(wide)
    dot = jnp.sum(by_out * wide, -1, keepdims=True)
    return (by_out * scale - wide * (scale * scale * scale * dot * (1 / wide.shape[-1]))).astype(BF16)


def _add(a, b):
    return (a.astype(F32) + b.astype(F32)).astype(BF16)


def _compact_body(got_ref, out_ref, *, count, rows):
    for i in range(count):
        out_ref[i * rows : (i + 1) * rows, :] = got_ref[i, :rows, :]


def compact(got, pieces, rows):
    count, _, width = got.shape
    return pl.pallas_call(
        functools.partial(_compact_body, count=count, rows=rows),
        grid=(pieces,),
        in_specs=[pl.BlockSpec((count, ROOM, width), lambda j: (0, j, 0))],
        out_specs=pl.BlockSpec((count * rows, width), lambda j: (0, j)),
        out_shape=jax.ShapeDtypeStruct((count * rows, pieces * width), BF16),
        compiler_params=_params(1),
        cost_estimate=_cost(2e9, 2 * got.size * 2),
        name="compact",
    )(got)


def _qkv_body(h_ref, w_ref, cos_ref, sin_ref, q_ref, k_ref, v_ref, a_ref, *, heads):
    wide = h_ref[...].astype(F32)
    a = (wide * _scale(wide)).astype(BF16)
    a_ref[...] = a
    cos, sin = cos_ref[...], sin_ref[...]
    out = _dot(a, w_ref[:, : (heads + 2) * HEAD]).astype(BF16)
    for n in range(heads + 1):
        t = out[:, n * HEAD : (n + 1) * HEAD].astype(F32)
        t = (t * cos + pltpu.roll(t, HEAD // 2, 1) * sin).astype(BF16)
        if n < heads:
            q_ref[n] = t
        else:
            k_ref[...] = t
    v_ref[...] = out[:, (heads + 1) * HEAD :]


def qkv_forward(h, w, at, heads, cos, sin, bm=512):
    s, d = h.shape
    rows = pl.BlockSpec((bm, d), lambda i: (i, 0))
    head = pl.BlockSpec((bm, HEAD), lambda i: (i, 0))
    wide = 1280
    return pl.pallas_call(
        functools.partial(_qkv_body, heads=heads),
        grid=(s // bm,),
        in_specs=[rows, _once((d, wide), (0, at // wide)), head, head],
        out_specs=[pl.BlockSpec((heads, bm, HEAD), lambda i: (0, i, 0)), head, head, rows],
        out_shape=[jax.ShapeDtypeStruct((heads, s, HEAD), BF16), jax.ShapeDtypeStruct((s, HEAD), BF16),
                   jax.ShapeDtypeStruct((s, HEAD), BF16), jax.ShapeDtypeStruct((s, d), BF16)],
        compiler_params=_params(1),
        cost_estimate=_cost(2 * s * d * (heads + 2) * HEAD, 16e6),
        name="qkv_forward",
    )(h, w, cos, sin)


def _qkv_back_body(dq_ref, dk_ref, dv_ref, h_ref, dh_ref, w_ref, cos_ref, sin_ref, all_ref, out_ref, *, heads):
    cos, sin = cos_ref[...], sin_ref[...]
    for n in range(heads + 1):
        t = (dq_ref[:, n * HEAD : (n + 1) * HEAD] if n < heads else dk_ref[...]).astype(F32)
        all_ref[:, n * HEAD : (n + 1) * HEAD] = (t * cos - pltpu.roll(t, HEAD // 2, 1) * sin).astype(BF16)
    all_ref[:, (heads + 1) * HEAD :] = dv_ref[...]
    da = _dot(all_ref[...], w_ref[:, : (heads + 2) * HEAD], 1, 1).astype(BF16).astype(F32)
    out_ref[...] = _add(dh_ref[...], _norm_back(da, h_ref[...].astype(F32)))


def qkv_backward(dq, dk, dv, h, dh, w, at, heads, cos, sin, bm=512):
    s, d = h.shape
    rows = pl.BlockSpec((bm, d), lambda i: (i, 0))
    head = pl.BlockSpec((bm, HEAD), lambda i: (i, 0))
    wide = 1280
    all_wide = (heads + 2) * HEAD
    return pl.pallas_call(
        functools.partial(_qkv_back_body, heads=heads),
        grid=(s // bm,),
        in_specs=[rows, head, head, rows, rows, _once((d, wide), (0, at // wide)), head, head],
        out_specs=[pl.BlockSpec((bm, all_wide), lambda i: (i, 0)), rows],
        out_shape=[jax.ShapeDtypeStruct((s, all_wide), BF16), jax.ShapeDtypeStruct((s, d), BF16)],
        compiler_params=_params(1),
        cost_estimate=_cost(2 * s * d * all_wide, 25e6),
        name="qkv_backward",
    )(dq, dk, dv, h, dh, w, cos, sin)


def _gap(bk, cols, bq):
    return lax.rem(lax.broadcasted_iota(jnp.int32, (bk, cols), 1), bq) - lax.broadcasted_iota(jnp.int32, (bk, cols), 0)


def _attend_body(q_ref, k_ref, v_ref, o_ref, lse_ref, top_s, mix_s, gap_s, *, scale, bq):
    g = q_ref.shape[0]
    cols = g * bq
    iq = pl.program_id(0)
    e = scale * LOG2E

    @pl.when(iq == 0)
    def _():
        gap_s[...] = _gap(bq // 2, bq, bq)

    top_s[...] = jnp.full((1, cols), NEG, F32)
    mix_s[...] = jnp.zeros((HEAD + 8, cols), F32)

    def block(start, count, first, masked):
        here = pl.ds(pl.multiple_of(start, count), count)
        keys = k_ref[here, :]
        scores = [_dot(keys, q_ref[n, first:, :], 1, 1) for n in range(g)]
        ok = gap_s[:, : bq - first] >= 0 if masked else None
        weights, keeps = [], []
        for n, s in enumerate(scores):
            at = slice(n * bq + first, (n + 1) * bq)
            if masked:
                s = jnp.where(ok, s, HIDDEN)
            old = top_s[:, at]
            top = jnp.maximum(old, s.max(axis=0, keepdims=True))
            top_s[:, at] = top
            weights.append(jnp.exp2((s - top) * e).astype(BF16))
            keeps.append(jnp.exp2((old - top) * e))
        values = jnp.concatenate([v_ref[here, :].T, jnp.ones((8, count), BF16)], axis=0)
        for n, (p, keep) in enumerate(zip(weights, keeps)):
            at = slice(n * bq + first, (n + 1) * bq)
            mix_s[:, at] = mix_s[:, at] * keep + _dot(values, p)

    lax.fori_loop(0, iq, lambda j, _: block(j * bq, bq, 0, False), None)
    block(iq * bq, bq // 2, 0, True)
    block(iq * bq + bq // 2, bq // 2, bq // 2, True)
    for n in range(g):
        at = slice(n * bq, (n + 1) * bq)
        total = mix_s[HEAD : HEAD + 1, at]
        o_ref[:, n * HEAD : (n + 1) * HEAD] = (mix_s[:HEAD, at] * (1 / total)).T.astype(BF16)
        lse_ref[n : n + 1, :] = top_s[:, at] * scale + jnp.log(total)


def attend(q, k, v, bq=512):
    g, s, d = q.shape
    whole = _once((s, d), (0, 0))
    return pl.pallas_call(
        functools.partial(_attend_body, scale=d**-0.5, bq=bq),
        grid=(s // bq,),
        in_specs=[pl.BlockSpec((g, bq, d), lambda i: (0, i, 0)), whole, whole],
        out_specs=[pl.BlockSpec((bq, g * d), lambda i: (i, 0)), pl.BlockSpec((g, bq), lambda i: (0, i))],
        out_shape=[jax.ShapeDtypeStruct((s, g * d), BF16), jax.ShapeDtypeStruct((g, s), F32)],
        scratch_shapes=[pltpu.VMEM((1, g * bq), F32), pltpu.VMEM((d + 8, g * bq), F32), pltpu.VMEM((bq // 2, bq), jnp.int32)],
        compiler_params=_params(1),
        cost_estimate=_cost(8 * g * s * s * d, 8e6, g * s * s),
        name="attend",
    )(q, k, v)


def _attend_back_body(q_ref, k_ref, v_ref, do_ref, o_ref, lse_ref, dq_ref, dk_ref, dv_ref, dq_s, dk_s, dv_s, gap_s, *, scale, bq):
    g = q_ref.shape[0]
    iq = pl.program_id(0)
    e = scale * LOG2E

    @pl.when(iq == 0)
    def _():
        gap_s[...] = _gap(bq // 2, bq, bq)
        dk_s[...] = jnp.zeros_like(dk_s)
        dv_s[...] = jnp.zeros_like(dv_s)

    dq_s[...] = jnp.zeros_like(dq_s)
    ones = jnp.ones((8, HEAD), BF16)
    lses, deltas = [], []
    for n in range(g):
        lses.append(lse_ref[n : n + 1, :] * LOG2E)
        both = do_ref[:, n * HEAD : (n + 1) * HEAD].astype(F32) * o_ref[:, n * HEAD : (n + 1) * HEAD].astype(F32)
        high = both.astype(BF16)
        rest = both - high.astype(F32)
        low = rest.astype(BF16)
        last = (rest - low.astype(F32)).astype(BF16)
        deltas.append((_dot(ones, high, 1, 1) + _dot(ones, low, 1, 1) + _dot(ones, last, 1, 1))[:1, :])

    def block(start, count, first, masked):
        here = pl.ds(pl.multiple_of(start, count), count)
        keys, values = k_ref[here, :], v_ref[here, :]
        qs = [q_ref[n, first:, :] for n in range(g)]
        dos = [do_ref[first:, n * HEAD : (n + 1) * HEAD] for n in range(g)]
        scores = [_dot(keys, x, 1, 1) for x in qs]
        dps = [_dot(values, x, 1, 1) for x in dos]
        ok = gap_s[:, : bq - first] >= 0 if masked else None
        turned = keys.T
        for n in range(g):
            p = jnp.exp2(scores[n] * e - lses[n][:, first:])
            if masked:
                p = jnp.where(ok, p, 0.0)
            ds = (p * (dps[n] - deltas[n][:, first:])).astype(BF16)
            dv_s[here, :] += _dot(p.astype(BF16), dos[n])
            dk_s[here, :] += _dot(ds, qs[n])
            dq_s[:, n * bq + first : (n + 1) * bq] += _dot(turned, ds)

    lax.fori_loop(0, iq, lambda j, _: block(j * bq, bq, 0, False), None)
    block(iq * bq, bq // 2, 0, True)
    block(iq * bq + bq // 2, bq // 2, bq // 2, True)
    for n in range(g):
        dq_ref[:, n * HEAD : (n + 1) * HEAD] = (dq_s[:, n * bq : (n + 1) * bq] * scale).T.astype(BF16)

    @pl.when(iq == pl.num_programs(0) - 1)
    def _():
        dk_ref[...] = (dk_s[...] * scale).astype(BF16)
        dv_ref[...] = dv_s[...].astype(BF16)


def attend_back(q, k, v, do, o, lse, bq=512):
    g, s, d = q.shape
    whole = _once((s, d), (0, 0))
    rows = pl.BlockSpec((bq, g * d), lambda i: (i, 0))
    return pl.pallas_call(
        functools.partial(_attend_back_body, scale=d**-0.5, bq=bq),
        grid=(s // bq,),
        in_specs=[pl.BlockSpec((g, bq, d), lambda i: (0, i, 0)), whole, whole, rows, rows, pl.BlockSpec((g, bq), lambda i: (0, i))],
        out_specs=[rows, pl.BlockSpec((s, d), lambda i: (0, 0)), pl.BlockSpec((s, d), lambda i: (0, 0))],
        out_shape=[jax.ShapeDtypeStruct((s, g * d), BF16), jax.ShapeDtypeStruct((s, d), BF16), jax.ShapeDtypeStruct((s, d), BF16)],
        scratch_shapes=[pltpu.VMEM((d, g * bq), F32), pltpu.VMEM((s, d), F32), pltpu.VMEM((s, d), F32), pltpu.VMEM((bq // 2, bq), jnp.int32)],
        compiler_params=_params(1),
        cost_estimate=_cost(10 * g * s * s * d, 16e6, g * s * s),
        name="attend_back",
    )(q, k, v, do, o, lse)


def _fetch_down(got_ref, down_s, sem, at, rows):
    @pl.when(pl.program_id(0) == 0)
    def _():
        copy = pltpu.make_async_copy(got_ref.at[:, pl.ds(at, rows), :], down_s, sem)
        copy.start()
        copy.wait()


def _mlp_body(o_ref, h_ref, gu_ref, wo_ref, got_ref, h2_ref, b_ref, g_ref, u_ref, act_ref, out_ref, down_s, sem, *, at, rows, part):
    _fetch_down(got_ref, down_s, sem, at, rows)
    ff = g_ref.shape[1]
    h2 = _add(h_ref[...], _dot(o_ref[...], wo_ref[...]).astype(BF16))
    h2_ref[...] = h2
    wide = h2.astype(F32)
    b = (wide * _scale(wide)).astype(BF16)
    b_ref[...] = b
    total = jnp.zeros(out_ref.shape, F32)
    step = part * rows
    for j in range(ff // step):
        here = slice(j * step, (j + 1) * step)
        gate = _dot(b, gu_ref[:, here])
        up = _dot(b, gu_ref[:, ff + j * step : ff + (j + 1) * step])
        g_ref[:, here] = gate
        u_ref[:, here] = up
        act = (gate * lax.logistic(gate) * up).astype(BF16)
        act_ref[:, here] = act
        total += _dot(act, down_s[j * part : (j + 1) * part].reshape(step, -1))
    out_ref[...] = _add(h2, total.astype(BF16))


def mlp_forward(o, h, w, got, at, rows, ff, bm=256, part=16):
    s, d = h.shape
    row = lambda n: pl.BlockSpec((bm, n), lambda i: (i, 0))
    sds = lambda n, t: jax.ShapeDtypeStruct((s, n), t)
    return pl.pallas_call(
        functools.partial(_mlp_body, at=at, rows=rows, part=part),
        grid=(s // bm,),
        in_specs=[row(d), row(d), _once((d, 2 * ff), (0, 0)), _once((d, d), (0, w.shape[1] // d - 1)), pl.BlockSpec(memory_space=pltpu.HBM)],
        out_specs=[row(d), row(d), row(ff), row(ff), row(ff), row(d)],
        out_shape=[sds(d, BF16), sds(d, BF16), sds(ff, F32), sds(ff, F32), sds(ff, BF16), sds(d, BF16)],
        scratch_shapes=[pltpu.VMEM((got.shape[0], rows, d), BF16), pltpu.SemaphoreType.DMA],
        compiler_params=_params(1),
        cost_estimate=_cost(2 * s * d * (3 * ff + d), 85e6, s * ff),
        name="mlp_forward",
    )(o, h, w, w, got)


def _mlp_back_body(dy_ref, g_ref, u_ref, h2_ref, gu_ref, wo_ref, got_ref, dg_ref, du_ref, dh_ref, do_ref, down_s, sem, *, at, rows, part):
    _fetch_down(got_ref, down_s, sem, at, rows)
    ff = g_ref.shape[1]
    dy = dy_ref[...]
    total = jnp.zeros(dh_ref.shape, F32)
    step = part * rows
    for j in range(ff // step):
        here = slice(j * step, (j + 1) * step)
        da = _dot(dy, down_s[j * part : (j + 1) * part].reshape(step, -1), 1, 1).astype(BF16).astype(F32)
        gate, up = g_ref[:, here], u_ref[:, here]
        s = lax.logistic(gate)
        dg = (da * up * (s * (1 + gate * (1 - s)))).astype(BF16)
        du = (da * (gate * s)).astype(BF16)
        dg_ref[:, here] = dg
        du_ref[:, here] = du
        total += _dot(dg, gu_ref[:, here], 1, 1) + _dot(du, gu_ref[:, ff + j * step : ff + (j + 1) * step], 1, 1)
    dh = _add(dy, _norm_back(total.astype(BF16).astype(F32), h2_ref[...].astype(F32)))
    dh_ref[...] = dh
    do_ref[...] = _dot(dh, wo_ref[...], 1, 1).astype(BF16)


def mlp_backward(dy, g, u, h2, w, got, at, rows, bm=256, part=16):
    s, d = dy.shape
    ff = g.shape[1]
    row = lambda n: pl.BlockSpec((bm, n), lambda i: (i, 0))
    sds = lambda n: jax.ShapeDtypeStruct((s, n), BF16)
    return pl.pallas_call(
        functools.partial(_mlp_back_body, at=at, rows=rows, part=part),
        grid=(s // bm,),
        in_specs=[row(d), row(ff), row(ff), row(d), _once((d, 2 * ff), (0, 0)), _once((d, d), (0, w.shape[1] // d - 1)),
                  pl.BlockSpec(memory_space=pltpu.HBM)],
        out_specs=[row(ff), row(ff), row(d), row(d)],
        out_shape=[sds(ff), sds(ff), sds(d), sds(d)],
        scratch_shapes=[pltpu.VMEM((got.shape[0], rows, d), BF16), pltpu.SemaphoreType.DMA],
        compiler_params=_params(1),
        cost_estimate=_cost(2 * s * d * (3 * ff + d), 95e6, s * ff),
        name="mlp_backward",
    )(dy, g, u, h2, w, w, got)


def _place(place_ref, i, value, keep_ref, send_ref, rows):
    at = place_ref[i]
    half = keep_ref.shape[0]

    @pl.when(at < half)
    def _():
        keep_ref[at, :rows, :] = value

    @pl.when(at >= half)
    def _():
        send_ref[at - half, :rows, :] = value


def _grad_wide_body(place_ref, a_ref, *rest, rows, steps, cut):
    *g_refs, keep_ref, send_ref, turned_s, sum_s = rest
    half, room, bn = keep_ref.shape

    @pl.when(pl.program_id(0) == 0)
    def _():
        turned_s[...] = a_ref[...].T

    def tile(g_ref, even_ref, odd_ref):
        if rows < room:
            blank = jnp.zeros((half, room - rows, bn), BF16)
            even_ref[:, rows:, :] = blank
            odd_ref[:, rows:, :] = blank
        turned = turned_s[...]
        for c in range(bn // cut):
            here = slice(c * cut, (c + 1) * cut)
            sum_s[c] = _dot(turned, g_ref[:, here])
            for i in range(2 * half):
                to = (even_ref, odd_ref)[i % 2]
                to[lax.rem(place_ref[i], half), :rows, here] = sum_s[c, i * rows : (i + 1) * rows, :].astype(BF16)

    even_first = place_ref[0] < half
    for n, g_ref in enumerate(g_refs):
        mine = lax.div(pl.program_id(0), steps) == n

        @pl.when(mine & even_first)
        def _():
            tile(g_ref, keep_ref, send_ref)

        @pl.when(mine & jnp.logical_not(even_first))
        def _():
            tile(g_ref, send_ref, keep_ref)


def grad_wide(place, a, *gs, rows, bn, cut):
    s, m = a.shape
    steps = gs[0].shape[1] // bn
    n = sum(g.shape[1] for g in gs)
    half = m // rows // 2
    out = pl.BlockSpec((half, ROOM, bn), lambda j, _: (0, 0, j))
    shape = jax.ShapeDtypeStruct((half, ROOM, n), BF16)
    ins = [pl.BlockSpec((s, bn), lambda j, _, i=i: (0, jnp.clip(j - i * steps, 0, steps - 1))) for i in range(len(gs))]
    return pl.pallas_call(
        functools.partial(_grad_wide_body, rows=rows, steps=steps, cut=cut),
        grid_spec=pltpu.PrefetchScalarGridSpec(
            num_scalar_prefetch=1, grid=(n // bn,),
            in_specs=[_once((s, m), (0, 0)), *ins],
            out_specs=[out, out],
            scratch_shapes=[pltpu.VMEM((m, s), BF16), pltpu.VMEM((bn // cut, m, cut), F32)]),
        out_shape=[shape, shape],
        compiler_params=_params(1),
        cost_estimate=_cost(2 * s * m * n, 2 * (s * m + s * n + m * n)),
        name="grad_wide",
    )(place, a, *gs)


def _grad_tall_body(place_ref, a_ref, g_ref, keep_ref, send_ref, sum_s, *, rows):
    sum_s[...] = _dot(a_ref[...].T, g_ref[...])
    count = sum_s.shape[0] // rows
    for i in range(count):
        _place(place_ref, pl.program_id(0) * count + i, sum_s[i * rows : (i + 1) * rows, :].astype(BF16), keep_ref, send_ref, rows)


def grad_tall(place, a, g, rows, bm):
    s, m = a.shape
    n = g.shape[1]
    half = m // rows // 2
    out = pl.BlockSpec((half, rows, n), lambda j, _: (0, 0, 0))
    shape = jax.ShapeDtypeStruct((half, rows, n), BF16)
    return pl.pallas_call(
        functools.partial(_grad_tall_body, rows=rows),
        grid_spec=pltpu.PrefetchScalarGridSpec(
            num_scalar_prefetch=1, grid=(m // bm,),
            in_specs=[pl.BlockSpec((s, bm), lambda j, _: (0, j)), _once((s, n), (0, 0))],
            out_specs=[out, out],
            scratch_shapes=[pltpu.VMEM((bm, n), F32)]),
        out_shape=[shape, shape],
        compiler_params=_params(1),
        cost_estimate=_cost(2 * s * m * n, 2 * (s * m + s * n + m * n)),
        name="grad_tall",
    )(place, a, g)


def solution(mesh):
    size = mesh.shape["dp"]
    CORE, ZNEAR, ZFAR, Y, X = 1, 2, 4, 8, 16
    ORDERS = {"gate_up": (CORE, X, Y, ZNEAR, ZFAR), "down": (CORE, ZNEAR, ZFAR, X, Y), "o": (CORE, X, Y, ZNEAR, ZFAR),
              "qkv": (CORE, X, Y, ZNEAR, ZFAR)}
    SPANS = {"gate_up": (1, 2, 2, 1, 1), "down": (1, 1, 2, 1, 1), "o": (1, 2, 1, 1, 1)}

    def place(order, me):
        away = jnp.arange(size, dtype=jnp.int32) ^ me
        at = jnp.zeros_like(away)
        for bit in order:
            at = 2 * at + ((away & bit) != 0)
        return at

    class Sums:
        def __init__(self):
            self.under_way, self.done, self.fresh, self.age, self.busy = {}, {}, [], {}, True

        def begin(self, name, order, keep, send):
            self.under_way[name], self.age[name] = [order, 0, keep, send, None], -1

        def advance(self):
            for name, state in list(self.under_way.items()):
                order, number, keep, send, got = state
                self.age[name] += 1
                if got is None or (self.busy and self.age[name] < SPANS.get(name[0], (1,) * 5)[number]):
                    continue
                self.age[name] = 0
                half = keep.shape[0] // 2
                if half == 0:
                    self.done[name] = _add(keep[0], got[0])
                    self.fresh.append(name)
                    del self.under_way[name]
                else:
                    self.under_way[name] = [order, number + 1, _add(keep[:half], got[:half]), _add(keep[half:], got[half:]), None]

        def fence(self, *values):
            names = [name for name, state in self.under_way.items() if state[4] is None]
            fresh, self.fresh = self.fresh, []
            values, halves, done = lax.optimization_barrier(
                (values, [self.under_way[name][2:4] for name in names], [self.done[name] for name in fresh]))
            self.done.update(zip(fresh, done))
            for name, (keep, send) in zip(names, halves):
                order, number = self.under_way[name][:2]
                got = lax.ppermute(send, "dp", [(i, i ^ order[number]) for i in range(size)])
                self.under_way[name] = [order, number, keep, send, got]
            return values

        def run(self, kernel, *values, **more):
            self.advance()
            return kernel(*self.fence(*values), **more)

        def finish(self):
            self.busy = False
            while self.under_way:
                self.advance()
                self.fence()

    def step(x, dy, wq, wk, wv, wo, w_gate, w_up, w_down):
        layers, own, d = wq.shape
        heads, ff, tall = wq.shape[2] // HEAD, w_gate.shape[2], w_down.shape[1]
        at_qkv = 2 * ff
        pieces = (2 * ff + wq.shape[2] + 2 * HEAD + d) // d
        s = x.shape[1]
        half = HEAD // 2
        angle = jnp.arange(s, dtype=F32)[:, None] * THETA ** (-jnp.arange(half, dtype=F32) / half)
        cos, sin = jnp.cos(angle), jnp.sin(angle)
        cos, sin = jnp.concatenate([cos, cos], 1), jnp.concatenate([-sin, sin], 1)

        gots = []
        for n in range(layers):
            rows = jnp.concatenate([w_gate[n], w_up[n], wq[n], wk[n], wv[n], wo[n]], 1).reshape(own, pieces, d)
            rows = jnp.pad(rows.transpose(1, 0, 2), ((0, 0), (0, ROOM - own), (0, 0))).reshape(pieces * ROOM, d)
            gots.append(lax.all_gather(jnp.concatenate([rows, w_down[n]], 0), "dp", axis=0))
        at_down = pieces * ROOM

        h, kept, ws = x[0], [], []
        for n in range(layers):
            w = compact(gots[n], pieces, own)
            q, k, v, a = qkv_forward(h, w, at_qkv, heads, cos, sin)
            o, lse = attend(q, k, v)
            h2, b, g, u, act, out = mlp_forward(o, h, w, gots[n], at_down, tall, ff)
            kept.append((h, q, k, v, a, o, lse, h2, b, g, u, act))
            ws.append(w)
            h = out

        me = lax.axis_index("dp")
        places = {name: place(order, me) for name, order in ORDERS.items()}
        by_h, sums = dy[0], Sums()

        def grad(name, n, kernel, *values, **more):
            sums.begin((name, n), ORDERS[name], *sums.run(functools.partial(kernel, places[name]), *values, **more))

        for n in reversed(range(layers)):
            h, q, k, v, a, o, lse, h2, b, g, u, act = kept[n]
            w, got = ws[n], gots[n]
            dg, du, dh, do = sums.run(mlp_backward, by_h, g, u, h2, w=w, got=got, at=at_down, rows=tall)
            grad("gate_up", n, grad_wide, b, dg, du, rows=own, bn=512, cut=512)
            grad("down", n, grad_tall, act, by_h, rows=tall, bm=640)
            grad("o", n, grad_wide, o, dh, rows=own, bn=896, cut=896)
            dq, dk, dv = sums.run(attend_back, q, k, v, do, o, lse)
            dqkv, by_h = sums.run(qkv_backward, dq, dk, dv, h, dh, w=w, at=at_qkv, heads=heads, cos=cos, sin=sin)
            grad("qkv", n, grad_wide, a, dqkv, rows=own, bn=384, cut=384)
        sums.finish()
        cut = heads * HEAD
        per = []
        for n in range(layers):
            qkv, gu = sums.done["qkv", n][:own], sums.done["gate_up", n][:own]
            per.append((qkv[:, :cut], qkv[:, cut : cut + HEAD], qkv[:, cut + HEAD :], sums.done["o", n][:own], gu[:, :ff], gu[:, ff:],
                        sums.done["down", n]))
        return (by_h[None], *(jnp.stack([p[i] for p in per]) for i in range(7)))

    states, cut = P(("rep", "dp"), None, None), P(None, "dp", None)
    return jax.shard_map(
        step,
        mesh=mesh,
        in_specs=(states, states) + (cut,) * 7,
        out_specs=(states,) + (P("rep", "dp", None),) * 7,
        check_vma=False,
    )
```
